32 devices in a mesh: dp: 8 (over z, x), mp: 4 (over y, core).
Axes of the slice: x: 2, y: 2, z: 4, core: 2. Of those that a mesh axis runs over, the one named last changes fastest.
Arguments:
- state_end: float32 [2048, 512], P('dp', 'mp'), may hold values from -6 to 6
- adjoint_end: float32 [2048, 512], P('dp', 'mp'), may hold values from -6 to 6
- increments: bfloat16 [8, 2048, 512], P(None, 'dp'), may hold values from -1.5 to 1.5
- w_in: bfloat16 [512, 2048], P(None, 'mp'), may hold values from -0.25 to 0.25
- b_in: float32 [2048], P('mp'), may hold values from -3 to 3
- w_out: bfloat16 [2048, 512], P('mp'), may hold values from -0.125 to 0.125
- b_out: float32 [512], replicated, may hold values from -3 to 3
- sigma: float32 [512], replicated, may hold values from 0.1 to 1
Outputs:
- state_start: float32 [2048, 512], P('dp', 'mp')
- adjoint_start: float32 [2048, 512], P('dp', 'mp')
- grad_w_in: float32 [512, 2048], P('dp', 'mp')
- grad_w_out: float32 [2048, 512], P('mp', 'dp')
The draws below stay inside these ranges and needn't reach their ends.
All inputs are finite; a program needn't handle non-finite values.
Results may differ from the reference program's by a relative error of at most 0.005.
Values may be sent and summed in bfloat16 or wider, within the bound.
A program may use at most 64 MiB of HBM per device.

```python
import math
import jax
import jax.numpy as jnp
from jax import lax

D = 512
H = 2048
STEPS = 8
BATCH = 2048


def shard_levels(stream_key, extent, cuts, least, top_value):
    level, own = 1.0, jax.random.fold_in(stream_key, 6)
    for dim, parts in cuts:
        steps = jnp.exp(jax.random.uniform(jax.random.fold_in(own, dim), (parts,), jnp.float32, least / len(cuts), top_value / len(cuts)))
        level = level * jnp.repeat(steps, extent[dim] // parts).reshape([-1 if axis == dim else 1 for axis in range(len(extent))])
    return level


def scatter_about(rng, extent, width, reach, cuts=(), held_as=jnp.bfloat16):
    values = jax.random.normal(rng, extent, jnp.float32) * width
    if len(cuts) > 0:
        values = shard_levels(rng, extent, cuts, -0.22, 0.18) * values
    return jnp.clip(values, min=-reach, max=reach).astype(held_as)


def setup_inputs(seed: int = 0) -> dict:
    arg_keys = jax.random.split(jax.random.key(seed), 9)
    return {
        "state_end": scatter_about(arg_keys[0], (BATCH, D), 1.0, 6.0, ((0, 8), (1, 4)), jnp.float32),
        "adjoint_end": scatter_about(arg_keys[1], (BATCH, D), 1.0, 6.0, ((0, 8), (1, 4)), jnp.float32),
        "increments": scatter_about(arg_keys[2], (STEPS, BATCH, D), 0.25, 1.5, ((1, 8),)),
        "w_in": scatter_about(arg_keys[3], (D, H), D ** -0.5, 0.25, ((1, 4),)),
        "b_in": scatter_about(arg_keys[4], (H,), 0.5, 3.0, ((0, 4),), jnp.float32),
        "w_out": scatter_about(arg_keys[5], (H, D), H ** -0.5, 0.125, ((0, 4),)),
        "b_out": scatter_about(arg_keys[6], (D,), 0.5, 3.0, (), jnp.float32),
        "sigma": jnp.clip(jnp.exp(jax.random.uniform(arg_keys[7], (D,), jnp.float32, math.log(0.1), math.log(1.0))), 0.1, 1.0),
    }


def reference(state_end, adjoint_end, increments, w_in, b_in, w_out, b_out, sigma):
    step_size = 1.0 / STEPS

    def advance(counter, carry):
        state, adjoint, acc_in, acc_out = carry
        level = (STEPS - 1 - counter).astype(jnp.int32)
        noise_now = lax.dynamic_index_in_dim(increments, level, 0, keepdims=False).astype(jnp.float32)
        z_low = state.astype(jnp.bfloat16)
        a_low = adjoint.astype(jnp.bfloat16)
        hidden = jnp.tanh(jnp.dot(z_low, w_in, preferred_element_type=jnp.float32) + b_in)
        hidden_low = hidden.astype(jnp.bfloat16)
        drift = jnp.dot(hidden_low, w_out, preferred_element_type=jnp.float32) + b_out
        back = jnp.dot(a_low, w_out.T, preferred_element_type=jnp.float32)
        delta = (back * (1.0 - hidden * hidden)).astype(jnp.bfloat16)
        pullback = jnp.dot(delta, w_in.T, preferred_element_type=jnp.float32)
        acc_in = acc_in + jnp.dot(z_low.T, delta, preferred_element_type=jnp.float32)
        acc_out = acc_out + jnp.dot(hidden_low.T, a_low, preferred_element_type=jnp.float32)
        adjoint = adjoint + step_size * pullback
        state = state - step_size * drift - sigma * noise_now
        return state, adjoint, acc_in, acc_out

    start = (state_end, adjoint_end, jnp.zeros((D, H), jnp.float32), jnp.zeros((H, D), jnp.float32))
    state, adjoint, acc_in, acc_out = lax.fori_loop(0, STEPS, advance, start)
    return state, adjoint, step_size * acc_in, step_size * acc_out
```

```python
import functools

import jax
import jax.numpy as jnp
from jax import lax
from jax.experimental import pallas as pl
from jax.experimental.pallas import tpu as pltpu
from jax.sharding import PartitionSpec as P

STEPS = 8
F32 = jnp.float32
LOW = jnp.bfloat16


def dot(x, y, cx, cy):
    return lax.dot_general(x, y, (((cx,), (cy,)), ((), ())), preferred_element_type=F32)


def kernel(
    mp, dp, state, adjoint, incr, w_in, b_in, w_out, b_out, sigma,
    state_o, adjoint_o, gin_o, gout_o,
    wi, wo, bi, rz, ra, noise, z_s, a_s, zall, aall, dall, hall,
    sz, sa, fz, fa, s1, r1, s2, r2, acc, s3, r3,
    sem_loc, sem_ws, sem_wf, sem_wr, sem_ss, sem_sr, sem_fs, sem_fr,
    sem_1s, sem_1r, sem_2s, sem_2r, sem_3s, sem_3r,
):
    step_size = 1.0 / STEPS
    m = lax.axis_index("mp")
    d = lax.axis_index("dp")
    ny = mp // 2
    y, c = m // 2, m % 2
    partner = y * 2 + (1 - c)
    rows = state.shape[0] // mp
    cols = state.shape[1]
    hs = w_in.shape[1]

    def remote(src, dst, ssem, rsem, axis, who):
        return pltpu.make_async_remote_copy(
            src_ref=src, dst_ref=dst, send_sem=ssem, recv_sem=rsem,
            device_id={axis: who}, device_id_type=pl.DeviceIdType.MESH)

    row0 = pl.multiple_of(m * rows, rows)
    loc = [
        pltpu.make_async_copy(incr.at[:, pl.ds(row0, rows), :], noise, sem_loc.at[0]),
        pltpu.make_async_copy(w_in, wi.at[m], sem_loc.at[1]),
        pltpu.make_async_copy(w_out, wo.at[m], sem_loc.at[2]),
    ]
    for q in loc:
        q.start()

    bar = pltpu.get_barrier_semaphore()
    for k in range(1, mp):
        pl.semaphore_signal(bar, inc=1, device_id={"mp": (m + k) % mp},
                            device_id_type=pl.DeviceIdType.MESH)
    for k in range(1, dp):
        pl.semaphore_signal(bar, inc=1, device_id={"dp": (d + k) % dp},
                            device_id_type=pl.DeviceIdType.MESH)
    pl.semaphore_wait(bar, mp - 1 + dp - 1)

    sends = []
    for k in range(1, mp):
        p = (m + k) % mp
        prow = pl.ds(pl.multiple_of(p * rows, rows), rows)
        for i, (src, dst) in enumerate(((state, rz), (adjoint, ra))):
            q = remote(src.at[prow, :], dst.at[m], sem_ss.at[i, k], sem_sr.at[i, m], "mp", p)
            q.start()
            sends.append(q)
    whole = ((b_in, bi), (w_in, wi), (w_out, wo))
    for k in range(1, ny):
        p = ((y + k) % ny) * 2 + c
        for i, (src, dst) in enumerate(whole):
            q = remote(src, dst.at[m], sem_ws.at[i, k], sem_wr.at[i, m], "mp", p)
            q.start()
            sends.append(q)
    for i, (src, dst) in enumerate(whole):
        q = remote(src, dst.at[m], sem_ws.at[i, 0], sem_wr.at[i, m], "mp", partner)
        q.start()
        sends.append(q)
    rz[m] = state[pl.ds(row0, rows), :]
    ra[m] = adjoint[pl.ds(row0, rows), :]
    bi[m] = b_in[...]
    for k in range(1, ny):
        slot = ((y + k) % ny) * 2 + c
        for i, (src, dst) in enumerate(whole):
            remote(src, dst.at[slot], sem_wf.at[i, k], sem_wr.at[i, slot], "mp", partner).wait_recv()
            q = remote(dst.at[slot], dst.at[slot], sem_wf.at[i, k], sem_wr.at[i, slot], "mp", partner)
            q.start()
            sends.append(q)
    for k in range(1, mp):
        p = (m + k) % mp
        for i, dst in enumerate((rz, ra)):
            remote(dst.at[p], dst.at[p], sem_ss.at[i, k], sem_sr.at[i, p], "mp", p).wait_recv()
    for q in loc:
        q.wait()
    z_s[...] = jnp.concatenate([rz[p] for p in range(mp)], axis=1)
    a_s[...] = jnp.concatenate([ra[p] for p in range(mp)], axis=1)
    for k in range(ny):
        slot = ((y + k) % ny) * 2 + (1 - c)
        for i, (src, dst) in enumerate(whole):
            remote(src, dst.at[slot], sem_ws.at[i, 0], sem_wr.at[i, slot], "mp", partner).wait_recv()
    for q in sends:
        q.wait_send()

    def advance(counter, carry):
        level = STEPS - 1 - counter
        at = pl.ds(pl.multiple_of(counter * rows, rows), rows)
        z, a = z_s[...], a_s[...]
        z_low, a_low = z.astype(LOW), a.astype(LOW)
        zall[at, :] = z_low
        aall[at, :] = a_low
        drift = b_out[...]
        pull = None
        for s in range(mp):
            hidden = jnp.tanh(dot(z_low, wi[s], 1, 0) + bi[s])
            back = dot(a_low, wo[s], 1, 1)
            hidden_low = hidden.astype(LOW)
            delta = (back * (1.0 - hidden * hidden)).astype(LOW)
            hall[s, at, :] = hidden_low
            dall[s, at, :] = delta
            drift = drift + dot(hidden_low, wo[s], 1, 0)
            part = dot(delta, wi[s], 1, 1)
            pull = part if pull is None else pull + part
        a_s[...] = a + step_size * pull
        z_s[...] = z - step_size * drift - sigma[...] * noise[level].astype(F32)
        return carry

    lax.fori_loop(0, STEPS, advance, 0)

    for p in range(mp):
        sz[p] = z_s[:, p * cols:(p + 1) * cols]
        sa[p] = a_s[:, p * cols:(p + 1) * cols]

    terms = ((zall, dall), (aall, hall))

    def term(i, s):
        x, v = terms[i]
        return dot(x[...], v[s], 0, 0)

    sends = []

    def to_partner(i, k):
        s = ((y + k) % ny) * 2 + (1 - c)
        s1[k, i] = term(i, s).astype(LOW)
        q = remote(s1.at[k, i], r1.at[k, i], sem_1s.at[k, i], sem_1r.at[k, i], "mp", partner)
        q.start()
        sends.append(q)

    def from_partner(i, k):
        remote(s1.at[k, i], r1.at[k, i], sem_1s.at[k, i], sem_1r.at[k, i], "mp", partner).wait_recv()

    for i in range(2):
        for k in range(1, ny):
            to_partner(i, k)
    for k in range(1, mp):
        p = (m + k) % mp
        for i, (src, dst) in enumerate(((sz, fz), (sa, fa))):
            q = remote(src.at[p], dst.at[m], sem_fs.at[i, k], sem_fr.at[i, m], "mp", p)
            q.start()
            sends.append(q)
    for i in range(2):
        for k in range(1, ny):
            own = term(i, ((y + k) % ny) * 2 + c)
            from_partner(i, k)
            s2[k, i] = (own + r1[k, i].astype(F32)).astype(LOW)
            q = remote(s2.at[k, i], r2.at[k, i], sem_2s.at[k, i], sem_2r.at[k, i],
                       "mp", ((y + k) % ny) * 2 + c)
            q.start()
            sends.append(q)
    for i in range(2):
        to_partner(i, 0)
    for i in range(2):
        acc[i] = term(i, m)
    for i in range(2):
        from_partner(i, 0)
        acc[i] = acc[i] + r1[0, i].astype(F32)
    state_o[pl.ds(row0, rows), :] = sz[m]
    adjoint_o[pl.ds(row0, rows), :] = sa[m]
    for k in range(1, mp):
        p = (m + k) % mp
        for i, (dst, out) in enumerate(((fz, state_o), (fa, adjoint_o))):
            remote(dst.at[p], dst.at[p], sem_fs.at[i, k], sem_fr.at[i, p], "mp", p).wait_recv()
            out[pl.ds(pl.multiple_of(p * rows, rows), rows), :] = dst[p]
    drows = acc.shape[1] // dp
    for i in range(2):
        for k in range(1, ny):
            remote(s2.at[k, i], r2.at[k, i], sem_2s.at[k, i], sem_2r.at[k, i], "mp", partner).wait_recv()
            acc[i] = acc[i] + r2[k, i].astype(F32)
        s3[i] = acc[i].astype(LOW).reshape(dp, drows, hs)
        for k in range(1, dp):
            p = (d + k) % dp
            q = remote(s3.at[i, p], r3.at[i, d], sem_3s.at[i, k], sem_3r.at[i, d], "dp", p)
            q.start()
            sends.append(q)
    for i in range(2):
        total = acc[i, pl.ds(pl.multiple_of(d * drows, drows), drows), :]
        for k in range(1, dp):
            p = (d + k) % dp
            remote(s3.at[i, p], r3.at[i, p], sem_3s.at[i, k], sem_3r.at[i, p], "dp", p).wait_recv()
            total = total + r3[i, p].astype(F32)
        total = total * step_size
        if i == 0:
            gin_o[...] = total
        else:
            gout_o[...] = total.T
    for q in sends:
        q.wait_send()


def body(mp, dp, state_end, adjoint_end, increments, w_in, b_in, w_out, b_out, sigma):
    br, cols = state_end.shape
    rows = br // mp
    width, hs = w_in.shape
    steps = increments.shape[0]
    ny = mp // 2
    drows = width // dp
    vm = pl.BlockSpec(memory_space=pltpu.VMEM)
    dma = pltpu.SemaphoreType.DMA
    scratch = [
        pltpu.VMEM((mp, width, hs), LOW),
        pltpu.VMEM((mp, hs, width), LOW),
        pltpu.VMEM((mp, 1, hs), F32),
        pltpu.VMEM((mp, rows, cols), F32),
        pltpu.VMEM((mp, rows, cols), F32),
        pltpu.VMEM((steps, rows, width), LOW),
        pltpu.VMEM((rows, width), F32),
        pltpu.VMEM((rows, width), F32),
        pltpu.VMEM((steps * rows, width), LOW),
        pltpu.VMEM((steps * rows, width), LOW),
        pltpu.VMEM((mp, steps * rows, hs), LOW),
        pltpu.VMEM((mp, steps * rows, hs), LOW),
        pltpu.VMEM((mp, rows, cols), F32),
        pltpu.VMEM((mp, rows, cols), F32),
        pltpu.VMEM((mp, rows, cols), F32),
        pltpu.VMEM((mp, rows, cols), F32),
        pltpu.VMEM((ny, 2, width, hs), LOW),
        pltpu.VMEM((ny, 2, width, hs), LOW),
        pltpu.VMEM((ny, 2, width, hs), LOW),
        pltpu.VMEM((ny, 2, width, hs), LOW),
        pltpu.VMEM((2, width, hs), F32),
        pltpu.VMEM((2, dp, drows, hs), LOW),
        pltpu.VMEM((2, dp, drows, hs), LOW),
        dma((3,)), dma((3, ny)), dma((3, ny)), dma((3, mp)),
        dma((2, mp)), dma((2, mp)), dma((2, mp)), dma((2, mp)),
        dma((ny, 2)), dma((ny, 2)), dma((ny, 2)), dma((ny, 2)),
        dma((2, dp)), dma((2, dp)),
    ]
    return pl.pallas_call(
        functools.partial(kernel, mp, dp),
        out_shape=(
            jax.ShapeDtypeStruct((br, cols), F32),
            jax.ShapeDtypeStruct((br, cols), F32),
            jax.ShapeDtypeStruct((drows, hs), F32),
            jax.ShapeDtypeStruct((hs, drows), F32),
        ),
        in_specs=[vm, vm, pl.BlockSpec(memory_space=pl.ANY), vm, vm, vm, vm, vm],
        out_specs=(vm, vm, vm, vm),
        scratch_shapes=scratch,
        compiler_params=pltpu.CompilerParams(
            collective_id=0, has_side_effects=True, vmem_limit_bytes=56 * 1024 * 1024),
    )(state_end, adjoint_end, increments, w_in, b_in.reshape(1, -1), w_out,
      b_out.reshape(1, -1), sigma.reshape(1, -1))


def solution(mesh):
    mp, dp = mesh.shape["mp"], mesh.shape["dp"]
    in_specs = (
        P("dp", "mp"),
        P("dp", "mp"),
        P(None, "dp", None),
        P(None, "mp"),
        P("mp"),
        P("mp", None),
        P(),
        P(),
    )
    out_specs = (P("dp", "mp"), P("dp", "mp"), P("dp", "mp"), P("mp", "dp"))
    return jax.shard_map(functools.partial(body, mp, dp), mesh=mesh, in_specs=in_specs,
                         out_specs=out_specs, check_vma=False)
```

```python
import functools

import jax
import jax.numpy as jnp
from jax import lax
from jax.experimental import pallas as pl
from jax.experimental.pallas import tpu as pltpu
from jax.sharding import PartitionSpec as P

STEPS = 8
CUTS = 2
COLS = 2
F32 = jnp.float32
LOW = jnp.bfloat16


def dot(x, y, cx, cy):
    return lax.dot_general(x, y, (((cx,), (cy,)), ((), ())), preferred_element_type=F32)


def kernel(
    mp, dp, state, adjoint, incr, w_in, b_in, w_out, b_out, sigma,
    state_o, adjoint_o, gin_o, gout_o,
    wi, wo, bi, rz, ra, noise, z_s, a_s, zall, aall, dall, hall,
    sz, sa, fz, fa, s1, r1, s2a, r2a, s2b, r2b, sxa, rxa, sxb, rxb, kb, half, acc, za, s3, r3,
    sem_loc, sem_ys, sem_xs, sem_ps, sem_ws, sem_wr, sem_bs, sem_br, sem_ss, sem_sr, sem_fs, sem_fr,
    sem_1s, sem_1r, sem_2s, sem_2r, sem_as, sem_ar, sem_cs, sem_cr, sem_3s, sem_3r,
):
    step_size = 1.0 / STEPS
    m = lax.axis_index("mp")
    d = lax.axis_index("dp")
    ny = mp // 2
    y, c = m // 2, m % 2
    partner = y * 2 + (1 - c)
    rows = state.shape[0] // mp
    cols = state.shape[1]
    hs = w_in.shape[1]

    def remote(src, dst, ssem, rsem, axis, who):
        return pltpu.make_async_remote_copy(
            src_ref=src, dst_ref=dst, send_sem=ssem, recv_sem=rsem,
            device_id={axis: who}, device_id_type=pl.DeviceIdType.MESH)

    row0 = pl.multiple_of(m * rows, rows)
    loc = [
        pltpu.make_async_copy(incr.at[:, pl.ds(row0, rows), :], noise, sem_loc.at[0]),
        pltpu.make_async_copy(w_in, wi.at[m], sem_loc.at[1]),
        pltpu.make_async_copy(w_out, wo.at[m], sem_loc.at[2]),
    ]
    for q in loc:
        q.start()

    bar = pltpu.get_barrier_semaphore()
    for k in range(1, mp):
        pl.semaphore_signal(bar, inc=1, device_id={"mp": (m + k) % mp},
                            device_id_type=pl.DeviceIdType.MESH)
    for k in range(1, dp):
        pl.semaphore_signal(bar, inc=1, device_id={"dp": (d + k) % dp},
                            device_id_type=pl.DeviceIdType.MESH)
    pl.semaphore_wait(bar, mp - 1 + dp - 1)

    sends = []

    def go(*args):
        q = remote(*args)
        q.start()
        sends.append(q)

    def share(p, k):
        prow = pl.ds(pl.multiple_of(p * rows, rows), rows)
        for i, (src, dst) in enumerate(((state, rz), (adjoint, ra))):
            go(src.at[prow, :], dst.at[m], sem_ss.at[i, k], sem_sr.at[i, m], "mp", p)

    h = d % 2
    beside = d + 1 - 2 * h
    weights = ((w_in, wi), (w_out, wo))
    span = w_in.shape[0] // (2 * CUTS)

    def piece(q):
        return pl.ds(pl.multiple_of(q * span, span), span)

    for j in range(CUTS):
        q = h * CUTS + j
        for i, (src, dst) in enumerate(weights):
            for k in range(1, ny):
                go(src.at[piece(q), :], dst.at[m, piece(q), :], sem_ys.at[i, k, j],
                   sem_wr.at[i, m, q], "mp", ((y + k) % ny) * 2 + c)
    share(partner, 0)
    for i, (src, dst) in enumerate(weights):
        go(src, dst.at[m], sem_ws.at[i], sem_wr.at[i, m, 0], "mp", partner)
    for k in range(1, mp):
        go(b_in, bi.at[m], sem_bs.at[k], sem_br.at[m], "mp", (m + k) % mp)
    for k in range(1, ny):
        for e in range(2):
            share(((y + k) % ny) * 2 + e, 2 * k + e)
    rz[m] = state[pl.ds(row0, rows), :]
    ra[m] = adjoint[pl.ds(row0, rows), :]
    bi[m] = b_in[...]

    def arrived(i, slot, q):
        dst = weights[i][1]
        ref = dst.at[slot, piece(q), :]
        remote(ref, ref, sem_ys.at[0, 0, 0], sem_wr.at[i, slot, q], "mp", partner).wait_recv()
        return ref

    def hand_on(i, k, half, j):
        slot = ((y + k) % ny) * 2 + c
        q = (h if half == 0 else 1 - h) * CUTS + j
        ref = arrived(i, slot, q)
        if half == 0:
            go(ref, ref, sem_xs.at[i, k, j], sem_wr.at[i, slot, q], "dp", beside)
        go(ref, ref, sem_ps.at[i, k, half * CUTS + j], sem_wr.at[i, slot, q], "mp", partner)

    order = [(i, j) for j in range(CUTS) for i in range(2)]
    for n in range(len(order) + 2):
        for k in range(1, ny):
            if n < len(order):
                hand_on(order[n][0], k, 0, order[n][1])
            if n >= 2:
                hand_on(order[n - 2][0], k, 1, order[n - 2][1])
    for k in range(1, mp):
        p = (m + k) % mp
        remote(b_in, bi.at[p], sem_bs.at[k], sem_br.at[p], "mp", p).wait_recv()
        for i, dst in enumerate((rz, ra)):
            remote(dst.at[p], dst.at[p], sem_ss.at[i, k], sem_sr.at[i, p], "mp", p).wait_recv()
    for q in loc:
        q.wait()
    z_s[...] = jnp.concatenate([rz[p] for p in range(mp)], axis=1)
    a_s[...] = jnp.concatenate([ra[p] for p in range(mp)], axis=1)
    for i, (src, dst) in enumerate(weights):
        remote(src, dst.at[partner], sem_ws.at[i], sem_wr.at[i, partner, 0], "mp", partner).wait_recv()
    for k in range(1, ny):
        for i in range(2):
            for q in range(2 * CUTS):
                arrived(i, ((y + k) % ny) * 2 + (1 - c), q)
    for q in sends:
        q.wait_send()

    def advance(counter, carry):
        level = STEPS - 1 - counter
        at = pl.ds(pl.multiple_of(counter * rows, rows), rows)
        z, a = z_s[...], a_s[...]
        z_low, a_low = z.astype(LOW), a.astype(LOW)
        zall[at, :] = z_low
        aall[at, :] = a_low
        drift = b_out[...]
        pull = None
        for s in range(mp):
            hidden = jnp.tanh(dot(z_low, wi[s], 1, 0) + bi[s])
            back = dot(a_low, wo[s], 1, 1)
            hidden_low = hidden.astype(LOW)
            delta = (back * (1.0 - hidden * hidden)).astype(LOW)
            hall[s, at, :] = hidden_low
            dall[s, at, :] = delta
            drift = drift + dot(hidden_low, wo[s], 1, 0)
            part = dot(delta, wi[s], 1, 1)
            pull = part if pull is None else pull + part
        a_s[...] = a + step_size * pull
        z_s[...] = z - step_size * drift - sigma[...] * noise[level].astype(F32)
        return carry

    lax.fori_loop(0, STEPS, advance, 0)

    for p in range(mp):
        sz[p] = z_s[:, p * cols:(p + 1) * cols]
        sa[p] = a_s[:, p * cols:(p + 1) * cols]

    terms = ((zall, dall), (aall, hall))
    dpq, cw = dp // 2, hs // COLS
    drows = w_in.shape[0] // dp
    quad = d // 2
    sends.clear()

    def over_y(k):
        return ((y + k) % ny) * 2 + c

    def landed(ref, sem):
        remote(ref, ref, sem_ys.at[0, 0, 0], sem, "mp", partner).wait_recv()
        return ref[...].astype(F32)

    def term(i, s, j):
        x, v = terms[i]
        return dot(x[...], v[s, :, j * cw:(j + 1) * cw], 0, 0)

    def to_partner(i, j, k):
        s1[i, j, k] = term(i, ((y + k) % ny) * 2 + (1 - c), j).astype(LOW)
        go(s1.at[i, j, k], r1.at[i, j, k], sem_1s.at[i, j, k], sem_1r.at[i, j, k], "mp", partner)

    def paired(i, j, k):
        own = term(i, over_y(k), j)
        return own + landed(r1.at[i, j, k], sem_1r.at[i, j, k])

    def split(value):
        half[...] = value.reshape(dpq, 2, drows, cw)
        return half[:, h], half[:, 1 - h]

    def first_y(j):
        for k in range(1, ny):
            s2a[j, k] = paired(0, j, k).astype(LOW)
            go(s2a.at[j, k], r2a.at[j, k], sem_2s.at[0, j, k], sem_2r.at[0, j, k], "mp", over_y(k))

    def first_x(j):
        value = acc[j]
        for k in range(1, ny):
            value = value + landed(r2a.at[j, k], sem_2r.at[0, j, k])
        keep, give = split(value)
        za[0, j] = keep
        sxa[j] = give.astype(LOW)
        go(sxa.at[j], rxa.at[j], sem_as.at[j], sem_ar.at[j], "dp", beside)

    def second_x(j):
        for k in range(ny):
            keep, give = split(paired(1, j, k))
            kb[j, k] = keep
            sxb[j, k] = give.astype(LOW)
            go(sxb.at[j, k], rxb.at[j, k], sem_cs.at[j, k], sem_cr.at[j, k], "dp", beside)

    def second_y(j):
        for k in list(range(1, ny)) + [0]:
            value = kb[j, k] + landed(rxb.at[j, k], sem_cr.at[j, k])
            if k == 0:
                za[1, j] = value
            else:
                s2b[j, k] = value.astype(LOW)
                go(s2b.at[j, k], r2b.at[j, k], sem_2s.at[1, j, k], sem_2r.at[1, j, k],
                   "mp", over_y(k))

    def last(i, j):
        value = za[i, j]
        if i == 0:
            value = value + landed(rxa.at[j], sem_ar.at[j])
        else:
            for k in range(1, ny):
                value = value + landed(r2b.at[j, k], sem_2r.at[1, j, k])
        za[i, j] = value
        s3[i, j] = value.astype(LOW)
        for k in range(1, dpq):
            p = (quad + k) % dpq
            go(s3.at[i, j, p], r3.at[i, j, quad], sem_3s.at[i, j, k], sem_3r.at[i, j, quad],
               "dp", p * 2 + h)

    for j in range(COLS):
        for k in range(1, ny):
            to_partner(0, j, k)
        for k in range(ny):
            to_partner(1, j, k)
        first_y(j)
        second_x(j)
    for j in range(COLS):
        to_partner(0, j, 0)
    for j in range(COLS):
        acc[j] = paired(0, j, 0)
    for j in range(COLS):
        first_x(j)
        second_y(j)
    for k in range(1, mp):
        p = (m + k) % mp
        for i, (src, dst) in enumerate(((sz, fz), (sa, fa))):
            go(src.at[p], dst.at[m], sem_fs.at[i, k], sem_fr.at[i, m], "mp", p)
    for j in range(COLS):
        for i in range(2):
            last(i, j)
    state_o[pl.ds(row0, rows), :] = sz[m]
    adjoint_o[pl.ds(row0, rows), :] = sa[m]
    for k in range(1, mp):
        p = (m + k) % mp
        for i, (dst, out) in enumerate(((fz, state_o), (fa, adjoint_o))):
            out[pl.ds(pl.multiple_of(p * rows, rows), rows), :] = landed(dst.at[p], sem_fr.at[i, p])
    for j in range(COLS):
        for i, out in enumerate((gin_o, gout_o)):
            total = za[i, j, quad]
            for k in range(1, dpq):
                p = (quad + k) % dpq
                total = total + landed(r3.at[i, j, p], sem_3r.at[i, j, p])
            out[:, j * cw:(j + 1) * cw] = total * step_size
    for q in sends:
        q.wait_send()


def place(*refs):
    for src, dst in zip(refs[:4], refs[4:]):
        dst[...] = src[...]


def body(mp, dp, state_end, adjoint_end, increments, w_in, b_in, w_out, b_out, sigma):
    br, cols = state_end.shape
    rows = br // mp
    width, hs = w_in.shape
    steps = increments.shape[0]
    ny = mp // 2
    drows = width // dp
    dpq, cw = dp // 2, hs // COLS
    vm = pl.BlockSpec(memory_space=pltpu.VMEM)
    dma = pltpu.SemaphoreType.DMA
    scratch = [
        pltpu.VMEM((mp, width, hs), LOW),
        pltpu.VMEM((mp, hs, width), LOW),
        pltpu.VMEM((mp, 1, hs), F32),
        pltpu.VMEM((mp, rows, cols), F32),
        pltpu.VMEM((mp, rows, cols), F32),
        pltpu.VMEM((steps, rows, width), LOW),
        pltpu.VMEM((rows, width), F32),
        pltpu.VMEM((rows, width), F32),
        pltpu.VMEM((steps * rows, width), LOW),
        pltpu.VMEM((steps * rows, width), LOW),
        pltpu.VMEM((mp, steps * rows, hs), LOW),
        pltpu.VMEM((mp, steps * rows, hs), LOW),
        pltpu.VMEM((mp, rows, cols), F32),
        pltpu.VMEM((mp, rows, cols), F32),
        pltpu.VMEM((mp, rows, cols), F32),
        pltpu.VMEM((mp, rows, cols), F32),
        pltpu.VMEM((2, COLS, ny, width, cw), LOW),
        pltpu.VMEM((2, COLS, ny, width, cw), LOW),
        pltpu.VMEM((COLS, ny, width, cw), LOW),
        pltpu.VMEM((COLS, ny, width, cw), LOW),
        pltpu.VMEM((COLS, ny, dpq, drows, cw), LOW),
        pltpu.VMEM((COLS, ny, dpq, drows, cw), LOW),
        pltpu.VMEM((COLS, dpq, drows, cw), LOW),
        pltpu.VMEM((COLS, dpq, drows, cw), LOW),
        pltpu.VMEM((COLS, ny, dpq, drows, cw), LOW),
        pltpu.VMEM((COLS, ny, dpq, drows, cw), LOW),
        pltpu.VMEM((COLS, ny, dpq, drows, cw), F32),
        pltpu.VMEM((dpq, 2, drows, cw), F32),
        pltpu.VMEM((COLS, width, cw), F32),
        pltpu.VMEM((2, COLS, dpq, drows, cw), F32),
        pltpu.VMEM((2, COLS, dpq, drows, cw), LOW),
        pltpu.VMEM((2, COLS, dpq, drows, cw), LOW),
        dma((3,)), dma((2, ny, CUTS)), dma((2, ny, CUTS)), dma((2, ny, 2 * CUTS)),
        dma((2,)), dma((2, mp, 2 * CUTS)), dma((mp,)), dma((mp,)),
        dma((2, mp)), dma((2, mp)), dma((2, mp)), dma((2, mp)),
        dma((2, COLS, ny)), dma((2, COLS, ny)), dma((2, COLS, ny)), dma((2, COLS, ny)),
        dma((COLS,)), dma((COLS,)), dma((COLS, ny)), dma((COLS, ny)),
        dma((2, COLS, dpq)), dma((2, COLS, dpq)),
    ]
    outs = pl.pallas_call(
        functools.partial(kernel, mp, dp),
        out_shape=(
            jax.ShapeDtypeStruct((br, cols), F32),
            jax.ShapeDtypeStruct((br, cols), F32),
            jax.ShapeDtypeStruct((drows, hs), F32),
            jax.ShapeDtypeStruct((drows, hs), F32),
        ),
        in_specs=[vm, vm, pl.BlockSpec(memory_space=pl.ANY), vm, vm, vm, vm, vm],
        out_specs=(vm, vm, vm, vm),
        scratch_shapes=scratch,
        compiler_params=pltpu.CompilerParams(
            collective_id=0, has_side_effects=True, vmem_limit_bytes=56 * 1024 * 1024),
    )(state_end, adjoint_end, increments, w_in, b_in.reshape(1, -1), w_out,
      b_out.reshape(1, -1), sigma.reshape(1, -1))
    state, adjoint, gin, gout = pl.pallas_call(
        place,
        out_shape=tuple(jax.ShapeDtypeStruct(o.shape, o.dtype) for o in outs),
        in_specs=[vm] * 4,
        out_specs=(vm,) * 4,
    )(*outs)
    return state, adjoint, gin, gout.T


def solution(mesh):
    mp, dp = mesh.shape["mp"], mesh.shape["dp"]
    in_specs = (
        P("dp", "mp"),
        P("dp", "mp"),
        P(None, "dp", None),
        P(None, "mp"),
        P("mp"),
        P("mp", None),
        P(),
        P(),
    )
    out_specs = (P("dp", "mp"), P("dp", "mp"), P("dp", "mp"), P("mp", "dp"))
    return jax.shard_map(functools.partial(body, mp, dp), mesh=mesh, in_specs=in_specs,
                         out_specs=out_specs, check_vma=False)
```
